128 devices in a mesh: dp: 64 (over z, y, x), tensor: 2 (over core).
Axes of the slice: x: 4, y: 4, z: 4, core: 2. Of those that a mesh axis runs over, the one named last changes fastest.
Arguments:
- encoded: bfloat16 [131072, 1152], P('dp', 'tensor'), may hold values from -9 to 9
- counts: int32 [2048], P('dp'), may hold values from 16 to 64
- win_ids: int32 [2048, 64], P('dp'), may hold values from 0 to 31, never falling along the last dimension, each value on 1 to 8 neighbouring positions
- dest_seq: int32 [2048], P('dp'), may hold values from 0 to 63, as said below
- dest_slot: int32 [2048], P('dp'), may hold values from 0 to 31, as said below
- w_first: bfloat16 [1152, 4608], P(None, 'tensor'), may hold values from -0.3125 to 0.3125
- b_first: float32 [4608], P('tensor'), may hold values from -3 to 3
- w_second: bfloat16 [4608, 2304], P('tensor'), may hold values from -0.1875 to 0.1875
- b_second: float32 [2304], P('tensor'), may hold values from -3 to 3
Outputs:
- projected: bfloat16 [65536, 2304], P('dp', 'tensor')
The draws below stay inside these ranges and needn't reach their ends.
Inputs may be any that keep to these rules, and one draw needn't show every extreme that they name: `dest_seq`: every sequence receives exactly 32 samples, no two of them from the same index of dp. `dest_slot`: the samples that one sequence receives have distinct block offsets.
All inputs are finite; a program needn't handle non-finite values.
Results may differ from the reference program's by a relative error of at most 0.009.
Values may be sent and summed in bfloat16 or wider, within the bound.
A program may use at most 128 MiB of HBM per device.

```python
import math
import jax
import jax.numpy as jnp
import numpy as np
from jax import lax

F = 1152
H = 4608
E = 2304
CAP = 64
BLOCK = 32
MOST = 8
SAMP_DEV = 32
SAMPLES = 2048
N_TENSOR = 2


def routing_tables(key):
    base = jax.random.fold_in(key, 11)
    key_outer, key_inner, key_shift, key_slots = jax.random.split(base, 4)
    groups = SAMPLES // SAMP_DEV
    outer_perm = jax.random.permutation(key_outer, groups)
    inner_perm = jax.random.permutation(key_inner, groups)
    shifts = jax.random.permutation(key_shift, groups)[:SAMP_DEV]
    sequence = outer_perm[(inner_perm[:, None] + shifts[None, :]) % groups]
    slot_table = jax.vmap(lambda single: jax.random.permutation(single, SAMP_DEV))(jax.random.split(key_slots, groups))
    slot_ids = slot_table[sequence, jnp.arange(SAMP_DEV)[None, :]]
    return (sequence.reshape(-1).astype(jnp.int32), slot_ids.reshape(-1).astype(jnp.int32))


def draw_dest_seq(key, part):
    return routing_tables(key)[0]


def draw_dest_slot(key, part):
    return routing_tables(key)[1]


def touch_ends(array, rng, least, largest):
    spot = [jax.random.randint(jax.random.fold_in(rng, axis), (), 0, length) for axis, length in enumerate(array.shape)]
    longest = array.shape.index(max(array.shape))
    beside = spot[:longest] + [(spot[longest] + 1) % array.shape[longest]] + spot[longest + 1:]
    return array.at[tuple(spot)].set(least).at[tuple(beside)].set(largest)


def with_spikes(result, stream_key, source, target, blocks, factor):
    owner, partner = [(jnp.arange(result.shape[dim]) // (result.shape[dim] // blocks)).reshape([-1 if axis == dim else 1 for axis in range(result.ndim)]) for dim in (source, target)]
    chosen = jax.random.permutation(stream_key, blocks)[partner]
    strong = (owner == chosen) | (owner == (partner + blocks // 2) % blocks)
    return jnp.where(strong, factor * result, result)


def shard_levels(key, dims, pieces, low, top_value):
    loudness = 1.0
    for dim, blocks in pieces:
        heights = jax.random.uniform(jax.random.fold_in(jax.random.fold_in(key, 6), dim), (blocks,), jnp.float32, low / len(pieces), top_value / len(pieces))
        loudness = loudness * jnp.repeat(jnp.exp(heights), dims[dim] // blocks).reshape((-1,) + (1,) * (len(dims) - 1 - dim))
    return loudness


def length_profile(count, total, most, lean):
    portions = [(1 << 20) // math.isqrt(rank ** lean) + 1 for rank in range(2, count + 1)]
    rest, given = total - most - (count - 1), [1] * (count - 1)
    while rest > 0:
        free = [i for i in range(count - 1) if given[i] < most]
        mass, remaining = sum([portions[i] for i in free]), rest
        for i in free:
            more = min(most - given[i], max(1, remaining * portions[i] // mass), rest)
            given[i] = given[i] + more
            rest = rest - more
    return np.array([most] + given)


def uneven(key, count, total, most, lean):
    if count == 2:
        one = jax.random.randint(key, (), max(1, total - most), min(most, total - 1) + 1)
        return jnp.stack([one, total - one])
    sizes = jnp.asarray(length_profile(count, total, most, lean), jnp.int32)
    pairs = (count - 1) // 2
    donor, sink = sizes[1:1 + 2 * pairs:2], sizes[2:2 + 2 * pairs:2]
    margin = jnp.minimum(donor - 1, most - sink)
    shifted = jax.random.randint(jax.random.fold_in(key, 1), (pairs,), 0, 1 << 20) % (margin + 1)
    sizes = sizes.at[1:1 + 2 * pairs:2].set(donor - shifted).at[2:2 + 2 * pairs:2].set(sink + shifted)
    return sizes[jax.random.permutation(jax.random.fold_in(key, 2), count)]


def bell_draw(own_key, shape, scale, reach, cuts=(), kind=jnp.bfloat16):
    loudness = shard_levels(own_key, shape, cuts, -0.22, 0.18) if cuts else 1.0
    drawn = jax.random.normal(own_key, shape, jnp.float32) * scale * loudness
    return jnp.minimum(jnp.maximum(drawn, -reach), reach).astype(kind)


def heavy_noise(rng, shape, spread, bound, cuts, heavy, held_as=jnp.bfloat16):
    drawn = spread * jax.random.normal(rng, shape, jnp.float32)
    if cuts:
        drawn = drawn * shard_levels(rng, shape, cuts, -0.22, 0.18)
    return jnp.clip(with_spikes(drawn, jax.random.fold_in(rng, 3), *heavy), -bound, bound).astype(held_as)


def setup_inputs(seed: int = 0) -> dict:
    streams_of = jax.random.split(jax.random.key(seed), 10)
    return {
        "encoded": bell_draw(streams_of[0], (SAMPLES * CAP, F), 1.5, 9.0, ((0, 64), (1, 2))),
        "counts": touch_ends(jax.random.randint(streams_of[1], (SAMPLES,), CAP // 4, CAP + 1), jax.random.fold_in(streams_of[1], 1), CAP // 4, CAP).astype(jnp.int32),
        "win_ids": jax.vmap(lambda own: jnp.searchsorted(jnp.cumsum(uneven(own, BLOCK, CAP, MOST, 1)), jnp.arange(CAP), side="right"))(jax.random.split(streams_of[2], SAMPLES)).reshape((SAMPLES, CAP)).astype(jnp.int32),
        "dest_seq": draw_dest_seq(jax.random.fold_in(streams_of[9], 71), 0),
        "dest_slot": draw_dest_slot(jax.random.fold_in(streams_of[9], 71), 0),
        "w_first": bell_draw(streams_of[5], (F, H), (F // 3) ** -0.5, 0.3125, ((1, 2),)),
        "b_first": bell_draw(streams_of[6], (H,), 0.5, 3.0, ((0, 2),), jnp.float32),
        "w_second": heavy_noise(streams_of[7], (H, E), (H // 2) ** -0.5, 0.1875, ((0, 2),), (0, 1, 2, 2.0)),
        "b_second": bell_draw(streams_of[8], (E,), 0.5, 3.0, ((0, 2),), jnp.float32),
    }


def reference(encoded, counts, win_ids, dest_seq, dest_slot, w_first, b_first, w_second, b_second):
    tokens = encoded.reshape(SAMPLES, CAP, F)
    positions = jnp.arange(CAP, dtype=jnp.int32)
    ids_live = jnp.where(positions[None, :] < counts[:, None], win_ids, -1)
    windows = jnp.arange(BLOCK, dtype=jnp.int32)
    onehot = (ids_live[:, None, :] == windows[None, :, None]).astype(jnp.float32)
    number = jnp.sum(onehot, axis=2)
    totals = jnp.einsum("nwc,ncf->nwf", onehot, tokens.astype(jnp.float32))
    pooled = (totals / jnp.maximum(number, 1.0)[:, :, None]).astype(jnp.bfloat16)
    position = (dest_seq * SAMP_DEV + dest_slot).astype(jnp.int32)
    packed = jnp.zeros((SAMPLES, BLOCK, F), jnp.bfloat16).at[position].set(pooled)
    packed = packed.reshape(SAMPLES * BLOCK, F)
    preact = jnp.dot(packed, w_first, preferred_element_type=jnp.float32) + b_first
    hidden = jax.nn.gelu(preact, approximate=True).astype(jnp.bfloat16)
    quota_size = H // N_TENSOR
    running = jnp.zeros((SAMPLES * BLOCK, E), jnp.float32)
    for member in range(N_TENSOR):
        portion = jnp.dot(hidden[:, member * quota_size:(member + 1) * quota_size],
                          w_second[member * quota_size:(member + 1) * quota_size],
                          preferred_element_type=jnp.float32).astype(jnp.bfloat16)
        portion = lax.optimization_barrier(portion)
        running = running + portion.astype(jnp.float32)
    return (running + b_second).astype(jnp.bfloat16)
```

```python
import functools

import jax
import jax.numpy as jnp
from jax import lax
from jax.experimental import pallas as pl
from jax.experimental.pallas import tpu as pltpu
from jax.sharding import PartitionSpec as P

MESH = pl.DeviceIdType.MESH
BF = jnp.bfloat16
F32 = jnp.float32
I32 = jnp.int32

GROUPS = 64
SAMP = 32
CAP = 64
BLOCK = 32
FH = 576
MAIN = 512
OUT = 1152
HID = 2304
CHUNKS = ((8, 0), (4, 16), (4, 24))
PAD = 640


def iota(shape, dim):
    return lax.broadcasted_iota(I32, shape, dim)


def target_of(me, step):
    off = lax.rem(step * 37, GROUPS)
    z = lax.rem(me // 16 + off // 16, 4)
    y = lax.rem(lax.rem(me // 4, 4) + lax.rem(off // 4, 4), 4)
    x = lax.rem(lax.rem(me, 4) + lax.rem(off, 4), 4)
    return z * 16 + y * 4 + x


def kernel(
    counts, dest_seq, dest_slot, win_ids, b_first, b_second, enc, w_first, w_second,
    out,
    tok, w1, w2, pooled0, pooled1, pooled2, snd0, snd1, snd2, arr0, arr1, arr2,
    meta_out, meta_in, xf0, xf1, xf2, hid, ps0, ps1, ps2, pr0, pr1, pr2, po,
    enc_sem, w_sem, meta_s, meta_r, a_s, a_r, x_s, x_r, p_s, p_r,
):
    me = lax.axis_index("dp")
    core = lax.axis_index("tensor")
    other = 1 - core
    pooled, snd, arr = (pooled0, pooled1, pooled2), (snd0, snd1, snd2), (arr0, arr1, arr2)
    xf, ps, pr = (xf0, xf1, xf2), (ps0, ps1, ps2), (pr0, pr1, pr2)

    barrier = pltpu.get_barrier_semaphore()

    def greet(step, _):
        pl.semaphore_signal(
            barrier, inc=1, device_id=(target_of(me, step), core), device_id_type=MESH
        )
        return 0

    lax.fori_loop(1, GROUPS, greet, 0)
    pl.semaphore_signal(barrier, inc=1, device_id=(me, other), device_id_type=MESH)

    enc_copy = pltpu.make_async_copy(enc, tok, enc_sem)
    enc_copy.start()

    w_copies = []
    for side, base in ((0, core * FH), (1, other * FH)):
        at = side * PAD
        w_copies += [(w_first.at[pl.ds(pl.multiple_of(base, 64), MAIN)], w1.at[pl.ds(at, MAIN)])]
        for twice in range(2):
            w_copies += [
                (
                    w_first.at[pl.ds(pl.multiple_of(base + MAIN, 64), 64)],
                    w1.at[pl.ds(at + MAIN + 64 * twice, 64)],
                )
            ]
    w_copies += [
        (w_second.at[:, pl.ds(pl.multiple_of(other * OUT, 128), OUT)], w2.at[:, pl.ds(0, OUT)]),
        (w_second.at[:, pl.ds(pl.multiple_of(core * OUT, 128), OUT)], w2.at[:, pl.ds(OUT, OUT)]),
    ]
    w_copies = [
        pltpu.make_async_copy(src, dst, w_sem.at[i]) for i, (src, dst) in enumerate(w_copies)
    ]

    row = iota((GROUPS, 128), 0)
    meta = jnp.zeros((GROUPS, 128), I32)
    for s in range(SAMP):
        meta = jnp.where(row == dest_seq[s], dest_slot[s] + 1, meta)
    meta_out[...] = meta.reshape(GROUPS, 1, 128)
    meta_in[pl.ds(me, 1)] = meta_out[pl.ds(me, 1)]

    ids = iota((SAMP, CAP), 1)
    srow = iota((SAMP, CAP), 0)
    limit = jnp.zeros((SAMP, CAP), I32)
    for s in range(SAMP):
        limit = jnp.where(srow == s, counts[s], limit)
    live = jnp.where(ids < limit, win_ids[...], -1)

    rho = iota((128, 256), 0)
    wmap = jnp.zeros((128, 256), I32)
    smap = jnp.zeros((128, 256), I32)
    base = 0
    for rows, first in CHUNKS:
        q = rho - base
        inside = (q >= 0) & (q < 8 * rows)
        h = q // (4 * rows)
        wmap = jnp.where(inside, first + h * rows + q % rows, wmap)
        smap = jnp.where(inside, (q // rows) % 4, smap)
        base += 8 * rows
    same = smap == iota((128, 256), 1) // CAP

    enc_copy.wait()
    for copy in w_copies:
        copy.start()

    for g in range(SAMP // 4):
        line = jnp.concatenate([live[4 * g + i : 4 * g + i + 1, :] for i in range(4)], axis=1)
        onehot = jnp.where((wmap == line) & same, 1.0, 0.0).astype(F32)
        number = jnp.sum(onehot, axis=1, keepdims=True)
        totals = lax.dot_general(
            onehot.astype(BF),
            tok[:, pl.ds(256 * g, 256)],
            (((1,), (1,)), ((), ())),
            preferred_element_type=F32,
        )
        mean = totals * (1.0 / jnp.maximum(number, 1.0))
        base = 0
        for c, (rows, _) in enumerate(CHUNKS):
            n = 4 * rows
            lo, hi = mean[base : base + n], mean[base + n : base + 2 * n]
            packed = jnp.concatenate(
                [lo[:, :MAIN], hi[:, :MAIN], lo[:, MAIN:], hi[:, MAIN:]], axis=1
            )
            pooled[c][pl.ds(n * g, n), :] = packed.astype(BF)
            base += 2 * n

    pl.semaphore_wait(barrier, GROUPS)

    def send_meta(step, _):
        to = target_of(me, step)
        pltpu.make_async_remote_copy(
            src_ref=meta_out.at[pl.ds(to, 1)],
            dst_ref=meta_in.at[pl.ds(me, 1)],
            send_sem=meta_s,
            recv_sem=meta_r,
            device_id=(to, core),
            device_id_type=MESH,
        ).start()
        return 0

    for c, (rows, _) in enumerate(CHUNKS):
        lanes = SAMP * rows
        where = jnp.zeros((8, lanes), I32)
        lane_s = iota((8, lanes), 1) // rows
        for s in range(SAMP):
            where = jnp.where(lane_s == s, dest_seq[s], where)
        shape = (GROUPS * rows, lanes)
        pick = (iota(shape, 0) // rows == where[0:1]) & (
            iota(shape, 0) % rows == iota(shape, 1) % rows
        )
        pick = jnp.where(pick, 1.0, 0.0).astype(BF)
        chosen = jnp.dot(pick, pooled[c][...], preferred_element_type=F32)
        snd[c][...] = chosen.reshape(GROUPS, rows, 2 * FH).astype(BF)
        arr[c][pl.ds(me, 1)] = snd[c][pl.ds(me, 1)]

        def send(step, _, c=c):
            to = target_of(me, step)
            pltpu.make_async_remote_copy(
                src_ref=snd[c].at[pl.ds(to, 1)],
                dst_ref=arr[c].at[pl.ds(me, 1)],
                send_sem=a_s.at[c],
                recv_sem=a_r.at[c],
                device_id=(to, core),
                device_id_type=MESH,
            ).start()
            return 0

        if c == 0:
            lax.fori_loop(1, GROUPS, send_meta, 0)
        lax.fori_loop(1, GROUPS, send, 0)

    def whole(src, dst, send_sem, recv_sem):
        return pltpu.make_async_remote_copy(
            src_ref=src.at[pl.ds(0, GROUPS - 1)],
            dst_ref=dst.at[pl.ds(0, GROUPS - 1)],
            send_sem=send_sem,
            recv_sem=recv_sem,
            device_id=(me, other),
            device_id_type=MESH,
        )

    def to_partner(src, dst, send_sem, recv_sem):
        return pltpu.make_async_remote_copy(
            src_ref=src,
            dst_ref=dst,
            send_sem=send_sem,
            recv_sem=recv_sem,
            device_id=(me, other),
            device_id_type=MESH,
        )

    whole(meta_out, meta_in, meta_s, meta_r).wait_recv()

    for c, (rows, first) in enumerate(CHUNKS):
        lanes = GROUPS * rows
        wins = 2 * rows
        total = SAMP * wins
        spread = jnp.where(iota((GROUPS, lanes), 1) // rows == iota((GROUPS, lanes), 0), 1.0, 0.0)
        slots = lax.dot_general(
            meta_in[...].reshape(GROUPS, 128).astype(F32).astype(BF),
            spread.astype(BF),
            (((0,), (0,)), ((), ())),
            preferred_element_type=F32,
        )
        shape = (total, lanes)
        mine = slots[0:1] == (iota(shape, 0) // wins + 1).astype(F32)
        win = iota(shape, 0) % wins
        lane_r = iota(shape, 1) % rows
        place = [
            jnp.where(mine & (win == h * rows + lane_r), 1.0, 0.0).astype(BF) for h in range(2)
        ]
        whole(snd[c], arr[c], a_s.at[c], a_r.at[c]).wait_recv()
        block = arr[c][...].reshape(lanes, 2 * FH)
        main = jnp.dot(place[0], block[:, :MAIN], preferred_element_type=F32) + jnp.dot(
            place[1], block[:, MAIN : 2 * MAIN], preferred_element_type=F32
        )
        tails = block[:, 2 * MAIN :]
        tail = jnp.where(
            iota((total, 128), 1) < FH - MAIN,
            jnp.dot(place[0], tails, preferred_element_type=F32),
            jnp.dot(place[1], tails, preferred_element_type=F32),
        )
        xf[c][:, pl.ds(0, MAIN)] = main.astype(BF)
        xf[c][:, pl.ds(MAIN, 128)] = tail.astype(BF)
        swap = to_partner(
            xf[c].at[:, pl.ds(0, PAD)], xf[c].at[:, pl.ds(PAD, PAD)], x_s.at[c], x_r.at[c]
        )
        swap.start()
        if c == 0:
            for copy in w_copies:
                copy.wait()
        swap.wait()

        def layer1(n, _, c=c, total=total):
            cols = pl.ds(pl.multiple_of(n * 256, 256), 256)
            pre = jnp.dot(xf[c][...], w1[:, cols], preferred_element_type=F32) + b_first[:, cols]
            hid[pl.ds(0, total), cols] = jax.nn.gelu(pre, approximate=True).astype(BF)
            return 0

        lax.fori_loop(0, HID // 256, layer1, 0)

        def layer2(n, _, c=c, total=total):
            cols = pl.ds(pl.multiple_of(n * 384, 128), 384)
            value = jnp.dot(
                hid[pl.ds(0, total), :], w2[:, cols], preferred_element_type=F32
            )
            ps[c][:, cols] = value.astype(BF)
            return 0

        lax.fori_loop(0, 3, layer2, 0)
        give = to_partner(ps[c], pr[c], p_s.at[c], p_r.at[c])
        give.start()

        def layer2own(n, _, total=total):
            cols = pl.ds(pl.multiple_of(n * 384, 128), 384)
            w_cols = pl.ds(pl.multiple_of(OUT + n * 384, 128), 384)
            value = jnp.dot(
                hid[pl.ds(0, total), :], w2[:, w_cols], preferred_element_type=F32
            )
            po[pl.ds(0, total), cols] = value.astype(BF)
            return 0

        lax.fori_loop(0, 3, layer2own, 0)
        give.wait()
        for n in range(3):
            cols = pl.ds(n * 384, 384)
            summed = po[pl.ds(0, total), cols].astype(F32) + pr[c][:, cols].astype(F32)
            value = (summed + b_second[:, cols]).reshape(SAMP, wins, 384)
            out[:, pl.ds(first, wins), cols] = value.astype(BF)

    whole(meta_out, meta_in, meta_s, meta_r).wait_send()
    for c in range(len(CHUNKS)):
        whole(snd[c], arr[c], a_s.at[c], a_r.at[c]).wait_send()


def shards(encoded, counts, win_ids, dest_seq, dest_slot, w_first, b_first, w_second, b_second):
    smem = pl.BlockSpec(memory_space=pltpu.SMEM)
    vmem = pl.BlockSpec(memory_space=pltpu.VMEM)
    hbm = pl.BlockSpec(memory_space=pl.ANY)
    n = len(CHUNKS)
    sizes = [rows for rows, _ in CHUNKS]
    scratch = [
        pltpu.VMEM((FH, SAMP * CAP), BF),
        pltpu.VMEM((2 * PAD, HID), BF),
        pltpu.VMEM((HID, 2 * OUT), BF),
    ]
    scratch += [pltpu.VMEM((SAMP * r, 2 * FH), BF) for r in sizes]
    scratch += [pltpu.VMEM((GROUPS, r, 2 * FH), BF) for r in sizes] * 2
    scratch += [pltpu.VMEM((GROUPS, 1, 128), I32)] * 2
    scratch += [pltpu.VMEM((SAMP * 2 * r, 2 * PAD), BF) for r in sizes]
    scratch += [pltpu.VMEM((SAMP * 2 * max(sizes), HID), BF)]
    scratch += [pltpu.VMEM((SAMP * 2 * r, OUT), BF) for r in sizes] * 2
    scratch += [pltpu.VMEM((SAMP * 2 * max(sizes), OUT), BF)]
    dma = pltpu.SemaphoreType.DMA
    scratch += [dma, dma((8,)), dma, dma, dma((n,)), dma((n,)), dma((n,)), dma((n,)), dma((n,)), dma((n,))]
    result = pl.pallas_call(
        kernel,
        name="pool_place_project",
        out_shape=jax.ShapeDtypeStruct((SAMP, BLOCK, OUT), BF),
        in_specs=[smem, smem, smem, vmem, vmem, vmem, hbm, hbm, hbm],
        out_specs=vmem,
        scratch_shapes=scratch,
        compiler_params=pltpu.CompilerParams(
            collective_id=0, has_side_effects=True, vmem_limit_bytes=52 << 20
        ),
    )(
        counts, dest_seq, dest_slot, win_ids, b_first.reshape(1, -1), b_second.reshape(1, -1),
        encoded.T, w_first, w_second,
    )
    return result.reshape(SAMP * BLOCK, OUT)


def solution(mesh):
    placed = (
        P("dp", "tensor"),
        P("dp"),
        P("dp", None),
        P("dp"),
        P("dp"),
        P(None, "tensor"),
        P("tensor"),
        P("tensor", None),
        P("tensor"),
    )
    return jax.shard_map(
        shards, mesh=mesh, in_specs=placed, out_specs=P("dp", "tensor"), check_vma=False
    )
```

```python
import functools

import jax
import jax.numpy as jnp
from jax import lax
from jax.experimental import pallas as pl
from jax.experimental.pallas import tpu as pltpu
from jax.sharding import PartitionSpec as P

MESH = pl.DeviceIdType.MESH
BF = jnp.bfloat16
F32 = jnp.float32
I32 = jnp.int32

GROUPS = 64
SAMP = 32
CAP = 64
BLOCK = 32
FH = 576
MAIN = 512
OUT = 1152
HID = 2304
CHUNKS = ((4, 0), (4, 8), (4, 16), (4, 24))
PAD = 640


def iota(shape, dim):
    return lax.broadcasted_iota(I32, shape, dim)


def div(x, n):
    return lax.shift_right_logical(x, jnp.int32(n.bit_length() - 1))


def mod(x, n):
    return lax.bitwise_and(x, jnp.int32(n - 1))


def peers(me):
    places = []
    for scale in (16, 4, 1):
        here = lax.rem(me // scale, 4)
        places.append([lax.rem(here + d, 4) * scale for d in range(4)])
    for step in range(1, GROUPS):
        off = step * 37 % GROUPS
        yield places[0][off // 16] + places[1][off // 4 % 4] + places[2][off % 4]


def gelu(x):
    half = 0.5 * x
    return half + half * jnp.tanh(x * (0.7978845608028654 + 0.035677408136300125 * (x * x)))


def kernel(*refs):
    n = len(CHUNKS)
    counts_in, seq_in, slot_in, win_in, b_first_in, b_second_in, enc, w_first, w_second, out = refs[:10]
    counts, dest_seq, dest_slot, win_ids, b_first, b_second, tok, w1, w2 = refs[10:19]
    meta_out, meta_in, hid, hot, scale = refs[19:24]
    pooled, snd, arr, xf, ps, pr, po, place, pick = (
        refs[24 + i * n : 24 + (i + 1) * n] for i in range(9)
    )
    in_sem, enc_sem, w_sem, meta_s, meta_r, a_s, a_r, x_s, x_r, p_s, p_r = refs[24 + 9 * n :]
    me = lax.axis_index("dp")
    core = lax.axis_index("tensor")
    other = 1 - core

    barrier = pltpu.get_barrier_semaphore()

    targets = list(peers(me))
    for to in targets:
        pl.semaphore_signal(barrier, inc=1, device_id=(to, core), device_id_type=MESH)
    pl.semaphore_signal(barrier, inc=1, device_id=(me, other), device_id_type=MESH)

    small = [
        pltpu.make_async_copy(src, dst, in_sem.at[i])
        for i, (src, dst) in enumerate(
            (
                (counts_in, counts),
                (seq_in, dest_seq),
                (slot_in, dest_slot),
                (win_in, win_ids),
                (b_first_in, b_first),
                (b_second_in, b_second),
            )
        )
    ]
    for copy in small:
        copy.start()
    enc_copy = pltpu.make_async_copy(enc, tok, enc_sem)
    enc_copy.start()

    w_copies = []
    for side, base in ((0, core * FH), (1, other * FH)):
        at = side * PAD
        w_copies += [(w_first.at[pl.ds(pl.multiple_of(base, 64), MAIN)], w1.at[pl.ds(at, MAIN)])]
        for twice in range(2):
            w_copies += [
                (
                    w_first.at[pl.ds(pl.multiple_of(base + MAIN, 64), 64)],
                    w1.at[pl.ds(at + MAIN + 64 * twice, 64)],
                )
            ]
    w_copies += [
        (w_second.at[:, pl.ds(pl.multiple_of(other * OUT, 128), OUT)], w2.at[:, pl.ds(0, OUT)]),
        (w_second.at[:, pl.ds(pl.multiple_of(core * OUT, 128), OUT)], w2.at[:, pl.ds(OUT, OUT)]),
    ]
    w_copies = [
        pltpu.make_async_copy(src, dst, w_sem.at[i]) for i, (src, dst) in enumerate(w_copies)
    ]

    for copy in small:
        copy.wait()
    row = iota((GROUPS, 128), 0)
    meta = jnp.zeros((GROUPS, 128), I32)
    for s in range(SAMP):
        meta = jnp.where(row == dest_seq[s], dest_slot[s] + 1, meta)
    meta_out[...] = meta.reshape(GROUPS, 1, 128)
    meta_in[pl.ds(me, 1)] = meta_out[pl.ds(me, 1)]

    ids = iota((SAMP, CAP), 1)
    srow = iota((SAMP, CAP), 0)
    limit = jnp.zeros((SAMP, CAP), I32)
    for s in range(SAMP):
        limit = jnp.where(srow == s, counts[s], limit)
    live = jnp.where(ids < limit, win_ids[...], -1)

    rho = iota((128, 256), 0)
    wmap = jnp.zeros((128, 256), I32)
    smap = jnp.zeros((128, 256), I32)
    base = 0
    for rows, first in CHUNKS:
        q = rho - base
        inside = (q >= 0) & (q < 8 * rows)
        h = div(q, 4 * rows)
        wmap = jnp.where(inside, first + h * rows + mod(q, rows), wmap)
        smap = jnp.where(inside, mod(div(q, rows), 4), smap)
        base += 8 * rows
    same = smap == div(iota((128, 256), 1), CAP)

    for g in range(SAMP // 4):
        line = jnp.concatenate([live[4 * g + i : 4 * g + i + 1, :] for i in range(4)], axis=1)
        onehot = jnp.where((wmap == line) & same, 1.0, 0.0).astype(F32)
        number = jnp.sum(onehot, axis=1, keepdims=True)
        hot[g] = onehot.astype(BF)
        scale[g] = jnp.broadcast_to(1.0 / jnp.maximum(number, 1.0), (128, 128))
    for c, (rows, _) in enumerate(CHUNKS):
        lanes = SAMP * rows
        where = jnp.zeros((8, lanes), I32)
        lane_s = div(iota((8, lanes), 1), rows)
        for s in range(SAMP):
            where = jnp.where(lane_s == s, dest_seq[s], where)
        shape = (GROUPS * rows, lanes)
        chosen = (div(iota(shape, 0), rows) == where[0:1]) & (
            mod(iota(shape, 0), rows) == mod(iota(shape, 1), rows)
        )
        pick[c][...] = jnp.where(chosen, 1.0, 0.0).astype(BF)

    enc_copy.wait()
    for copy in w_copies:
        copy.start()

    for g in range(SAMP // 4):
        totals = lax.dot_general(
            hot[g],
            tok[:, pl.ds(256 * g, 256)],
            (((1,), (1,)), ((), ())),
            preferred_element_type=F32,
        )
        mean = totals * scale[g][:, 0:1]
        base = 0
        for c, (rows, _) in enumerate(CHUNKS):
            n = 4 * rows
            lo, hi = mean[base : base + n], mean[base + n : base + 2 * n]
            packed = jnp.concatenate(
                [lo[:, :MAIN], hi[:, :MAIN], lo[:, MAIN:], hi[:, MAIN:]], axis=1
            )
            pooled[c][pl.ds(n * g, n), :] = packed.astype(BF)
            base += 2 * n

    def choose(c):
        rows = CHUNKS[c][0]
        chosen = jnp.dot(pick[c][...], pooled[c][...], preferred_element_type=F32)
        snd[c][...] = chosen.reshape(GROUPS, rows, 2 * FH).astype(BF)
        arr[c][pl.ds(me, 1)] = snd[c][pl.ds(me, 1)]

    def send_all(src, dst, send_sem, recv_sem):
        for to in targets:
            pltpu.make_async_remote_copy(
                src_ref=src.at[pl.ds(to, 1)],
                dst_ref=dst.at[pl.ds(me, 1)],
                send_sem=send_sem,
                recv_sem=recv_sem,
                device_id=(to, core),
                device_id_type=MESH,
            ).start()

    choose(0)
    pl.semaphore_wait(barrier, GROUPS)
    send_all(meta_out, meta_in, meta_s, meta_r)
    send_all(snd[0], arr[0], a_s.at[0], a_r.at[0])
    for c in range(1, len(CHUNKS)):
        choose(c)
        send_all(snd[c], arr[c], a_s.at[c], a_r.at[c])

    def whole(src, dst, send_sem, recv_sem):
        return pltpu.make_async_remote_copy(
            src_ref=src.at[pl.ds(0, GROUPS - 1)],
            dst_ref=dst.at[pl.ds(0, GROUPS - 1)],
            send_sem=send_sem,
            recv_sem=recv_sem,
            device_id=(me, other),
            device_id_type=MESH,
        )

    def to_partner(src, dst, send_sem, recv_sem):
        return pltpu.make_async_remote_copy(
            src_ref=src,
            dst_ref=dst,
            send_sem=send_sem,
            recv_sem=recv_sem,
            device_id=(me, other),
            device_id_type=MESH,
        )

    whole(meta_out, meta_in, meta_s, meta_r).wait_recv()

    for c, (rows, _) in enumerate(CHUNKS):
        lanes = GROUPS * rows
        wins = 2 * rows
        spread = jnp.where(
            div(iota((GROUPS, lanes), 1), rows) == iota((GROUPS, lanes), 0), 1.0, 0.0
        )
        slots = lax.dot_general(
            meta_in[...].reshape(GROUPS, 128).astype(F32).astype(BF),
            spread.astype(BF),
            (((0,), (0,)), ((), ())),
            preferred_element_type=F32,
        )
        shape = (SAMP * wins, lanes)
        mine = slots[0:1] == (div(iota(shape, 0), wins) + 1).astype(F32)
        win = mod(iota(shape, 0), wins)
        lane_r = mod(iota(shape, 1), rows)
        for h in range(2):
            place[c][h] = jnp.where(mine & (win == h * rows + lane_r), 1.0, 0.0).astype(BF)

    def gather(c):
        rows = CHUNKS[c][0]
        lanes = GROUPS * rows
        total = SAMP * 2 * rows
        whole(snd[c], arr[c], a_s.at[c], a_r.at[c]).wait_recv()
        block = arr[c][...].reshape(lanes, 2 * FH)
        main = jnp.dot(place[c][0], block[:, :MAIN], preferred_element_type=F32) + jnp.dot(
            place[c][1], block[:, MAIN : 2 * MAIN], preferred_element_type=F32
        )
        tails = block[:, 2 * MAIN :]
        tail = jnp.where(
            iota((total, 128), 1) < FH - MAIN,
            jnp.dot(place[c][0], tails, preferred_element_type=F32),
            jnp.dot(place[c][1], tails, preferred_element_type=F32),
        )
        xf[c][:, pl.ds(0, MAIN)] = main.astype(BF)
        xf[c][:, pl.ds(MAIN, 128)] = tail.astype(BF)
        swap = to_partner(
            xf[c].at[:, pl.ds(0, PAD)], xf[c].at[:, pl.ds(PAD, PAD)], x_s.at[c], x_r.at[c]
        )
        swap.start()
        return swap

    def layer1(c):
        total = SAMP * 2 * CHUNKS[c][0]
        for n in range(HID // 256):
            cols = pl.ds(n * 256, 256)
            pre = jnp.dot(xf[c][...], w1[:, cols], preferred_element_type=F32)
            pre = pre + b_first[cols].reshape(1, 256)
            hid[pl.ds(0, total), cols] = gelu(pre).astype(BF)

    def layer2(c, tiles):
        total = SAMP * 2 * CHUNKS[c][0]
        for n in tiles:
            cols = pl.ds(n * 256, 256)
            value = jnp.dot(hid[pl.ds(0, total), :], w2[:, cols], preferred_element_type=F32)
            value = value.astype(BF)
            if n < 4:
                ps[c][:, cols] = value
            elif n == 4:
                ps[c][:, pl.ds(1024, 128)] = value[:, :128]
                po[c][:, pl.ds(0, 128)] = value[:, 128:]
            else:
                po[c][:, pl.ds(n * 256 - OUT, 256)] = value

    def finish(c):
        rows, first = CHUNKS[c]
        for n in range(3):
            cols = pl.ds(n * 384, 384)
            summed = po[c][:, cols].astype(F32) + pr[c][:, cols].astype(F32)
            value = (summed + b_second[cols].reshape(1, 384)).reshape(SAMP, 2 * rows, 384)
            out[:, pl.ds(first, 2 * rows), cols] = value.astype(BF)

    swap = gather(0)
    for copy in w_copies:
        copy.wait()
    pending = None
    for c in range(len(CHUNKS)):
        last = c == len(CHUNKS) - 1
        if pending is not None:
            pending.wait()
            finish(c - 1)
        swap.wait()
        layer1(c)
        layer2(c, range(5))
        give = to_partner(ps[c], pr[c], p_s.at[c], p_r.at[c])
        give.start()
        if not last:
            swap = gather(c + 1)
        layer2(c, range(5, 9))
        pending = give
    pending.wait()
    finish(len(CHUNKS) - 1)

    whole(meta_out, meta_in, meta_s, meta_r).wait_send()
    for c in range(len(CHUNKS)):
        whole(snd[c], arr[c], a_s.at[c], a_r.at[c]).wait_send()


def shards(encoded, counts, win_ids, dest_seq, dest_slot, w_first, b_first, w_second, b_second):
    vmem = pl.BlockSpec(memory_space=pltpu.VMEM)
    hbm = pl.BlockSpec(memory_space=pltpu.HBM)
    n = len(CHUNKS)
    sizes = [rows for rows, _ in CHUNKS]
    scratch = [pltpu.SMEM((SAMP,), I32)] * 3
    scratch += [
        pltpu.VMEM((SAMP, CAP), I32),
        pltpu.VMEM((HID,), F32),
        pltpu.VMEM((OUT,), F32),
        pltpu.VMEM((FH, SAMP * CAP), BF),
        pltpu.VMEM((2 * PAD, HID), BF),
        pltpu.VMEM((HID, 2 * OUT), BF),
    ]
    scratch += [pltpu.VMEM((GROUPS, 1, 128), I32)] * 2
    scratch += [pltpu.VMEM((SAMP * 2 * max(sizes), HID), BF)]
    scratch += [pltpu.VMEM((SAMP // 4, 128, 256), BF), pltpu.VMEM((SAMP // 4, 128, 128), F32)]
    scratch += [pltpu.VMEM((SAMP * r, 2 * FH), BF) for r in sizes]
    scratch += [pltpu.VMEM((GROUPS, r, 2 * FH), BF) for r in sizes] * 2
    scratch += [pltpu.VMEM((SAMP * 2 * r, 2 * PAD), BF) for r in sizes]
    scratch += [pltpu.VMEM((SAMP * 2 * r, OUT), BF) for r in sizes] * 3
    scratch += [pltpu.VMEM((2, SAMP * 2 * r, GROUPS * r), BF) for r in sizes]
    scratch += [pltpu.VMEM((GROUPS * r, SAMP * r), BF) for r in sizes]
    dma = pltpu.SemaphoreType.DMA
    scratch += [dma((6,)), dma, dma((8,)), dma, dma, dma((n,)), dma((n,)), dma((n,)), dma((n,)), dma((n,)), dma((n,))]
    result = pl.pallas_call(
        kernel,
        name="pool_place_project",
        out_shape=pltpu.VMEM((SAMP, BLOCK, OUT), BF),
        in_specs=[hbm] * 9,
        out_specs=vmem,
        scratch_shapes=scratch,
        compiler_params=pltpu.CompilerParams(
            collective_id=0, has_side_effects=True, vmem_limit_bytes=52 << 20
        ),
    )(
        counts, dest_seq, dest_slot, win_ids, b_first, b_second,
        encoded.T, w_first, w_second,
    )
    return result.reshape(SAMP * BLOCK, OUT)


def solution(mesh):
    placed = (
        P("dp", "tensor"),
        P("dp"),
        P("dp", None),
        P("dp"),
        P("dp"),
        P(None, "tensor"),
        P("tensor"),
        P("tensor", None),
        P("tensor"),
    )
    return jax.shard_map(
        shards, mesh=mesh, in_specs=placed, out_specs=P("dp", "tensor"), check_vma=False
    )
```

```python
import functools

import jax
import jax.numpy as jnp
from jax import lax
from jax.experimental import pallas as pl
from jax.experimental.pallas import tpu as pltpu
from jax.sharding import PartitionSpec as P

MESH = pl.DeviceIdType.MESH
BF = jnp.bfloat16
F32 = jnp.float32
I32 = jnp.int32

GROUPS = 64
SAMP = 32
CAP = 64
BLOCK = 32
FH = 576
MAIN = 512
OUT = 1152
HID = 2304
CHUNKS = tuple((2, 4 * c) for c in range(8))
EARLY = 8
PAD = 640


def iota(shape, dim):
    return lax.broadcasted_iota(I32, shape, dim)


def div(x, n):
    return lax.shift_right_logical(x, jnp.int32(n.bit_length() - 1))


def mod(x, n):
    return lax.bitwise_and(x, jnp.int32(n - 1))


def hops(off):
    return sum(min(d, 4 - d) for d in off)


def peers(me):
    places = []
    for scale in (16, 4, 1):
        here = lax.rem(me // scale, 4)
        places.append([lax.rem(here + d, 4) * scale for d in range(4)])
    offsets = [(i // 16, i // 4 % 4, i % 4) for i in range(1, GROUPS)]
    done = []
    for off in sorted(offsets, key=lambda o: -hops(o)):
        for one in (off, tuple((4 - d) % 4 for d in off)):
            if one not in done:
                done.append(one)
    return [sum(places[i][d] for i, d in enumerate(off)) for off in done]


def gelu(x):
    half = 0.5 * x
    return half + half * jnp.tanh(x * (0.7978845608028654 + 0.035677408136300125 * (x * x)))


def kernel(*refs):
    n = len(CHUNKS)
    counts_in, seq_in, slot_in, win_in, b_first_in, b_second_in, enc, w_first, w_second, out = refs[:10]
    counts, dest_seq, dest_slot, win_ids, b_first, b_second, tok, w1, w2 = refs[10:19]
    meta_out, meta_in, hid, hot, scale = refs[19:24]
    pooled, snd, arr, xf, ps, pr, po, place, pick = (
        refs[24 + i * n : 24 + (i + 1) * n] for i in range(9)
    )
    in_sem, enc_sem, w_sem, meta_s, meta_r, a_s, a_r, x_s, x_r, p_s, p_r = refs[24 + 9 * n :]
    me = lax.axis_index("dp")
    core = lax.axis_index("tensor")
    other = 1 - core

    barrier = pltpu.get_barrier_semaphore()

    targets = peers(me)
    for to in targets:
        pl.semaphore_signal(barrier, inc=1, device_id=(to, core), device_id_type=MESH)
    pl.semaphore_signal(barrier, inc=1, device_id=(me, other), device_id_type=MESH)

    small = [
        pltpu.make_async_copy(src, dst, in_sem.at[i])
        for i, (src, dst) in enumerate(
            (
                (counts_in, counts),
                (seq_in, dest_seq),
                (slot_in, dest_slot),
                (win_in, win_ids),
                (b_first_in, b_first),
                (b_second_in, b_second),
            )
        )
    ]
    for copy in small:
        copy.start()
    enc_copy = pltpu.make_async_copy(enc, tok, enc_sem)
    enc_copy.start()

    w_copies = []
    for side, base in ((0, core * FH), (1, other * FH)):
        at = side * PAD
        w_copies += [(w_first.at[pl.ds(pl.multiple_of(base, 64), MAIN)], w1.at[pl.ds(at, MAIN)])]
        for twice in range(2):
            w_copies += [
                (
                    w_first.at[pl.ds(pl.multiple_of(base + MAIN, 64), 64)],
                    w1.at[pl.ds(at + MAIN + 64 * twice, 64)],
                )
            ]
    w_copies += [
        (w_second.at[:, pl.ds(pl.multiple_of(other * OUT, 128), OUT)], w2.at[:, pl.ds(0, OUT)]),
        (w_second.at[:, pl.ds(pl.multiple_of(core * OUT, 128), OUT)], w2.at[:, pl.ds(OUT, OUT)]),
    ]
    w_copies = [
        pltpu.make_async_copy(src, dst, w_sem.at[i]) for i, (src, dst) in enumerate(w_copies)
    ]

    for copy in small:
        copy.wait()
    row = iota((GROUPS, 128), 0)
    meta = jnp.zeros((GROUPS, 128), I32)
    for s in range(SAMP):
        meta = jnp.where(row == dest_seq[s], dest_slot[s] + 1, meta)
    meta_out[...] = meta.reshape(GROUPS, 1, 128)
    meta_in[pl.ds(me, 1)] = meta_out[pl.ds(me, 1)]

    ids = iota((SAMP, CAP), 1)
    srow = iota((SAMP, CAP), 0)
    limit = jnp.zeros((SAMP, CAP), I32)
    for s in range(SAMP):
        limit = jnp.where(srow == s, counts[s], limit)
    live = jnp.where(ids < limit, win_ids[...], -1)

    rho = iota((128, 256), 0)
    wmap = jnp.zeros((128, 256), I32)
    smap = jnp.zeros((128, 256), I32)
    base = 0
    for rows, first in CHUNKS:
        q = rho - base
        inside = (q >= 0) & (q < 8 * rows)
        h = div(q, 4 * rows)
        wmap = jnp.where(inside, first + h * rows + mod(q, rows), wmap)
        smap = jnp.where(inside, mod(div(q, rows), 4), smap)
        base += 8 * rows
    same = smap == div(iota((128, 256), 1), CAP)

    for g in range(SAMP // 4):
        line = jnp.concatenate([live[4 * g + i : 4 * g + i + 1, :] for i in range(4)], axis=1)
        onehot = jnp.where((wmap == line) & same, 1.0, 0.0).astype(F32)
        number = jnp.sum(onehot, axis=1, keepdims=True)
        hot[g] = onehot.astype(BF)
        scale[g] = jnp.broadcast_to(1.0 / jnp.maximum(number, 1.0), (128, 128))
    for c, (rows, _) in enumerate(CHUNKS):
        lanes = SAMP * rows
        where = jnp.zeros((8, lanes), I32)
        lane_s = div(iota((8, lanes), 1), rows)
        for s in range(SAMP):
            where = jnp.where(lane_s == s, dest_seq[s], where)
        shape = (GROUPS * rows, lanes)
        chosen = (div(iota(shape, 0), rows) == where[0:1]) & (
            mod(iota(shape, 0), rows) == mod(iota(shape, 1), rows)
        )
        pick[c][...] = jnp.where(chosen, 1.0, 0.0).astype(BF)

    enc_copy.wait()
    for copy in w_copies:
        copy.start()

    for g in range(SAMP // 4):
        totals = lax.dot_general(
            hot[g],
            tok[:, pl.ds(256 * g, 256)],
            (((1,), (1,)), ((), ())),
            preferred_element_type=F32,
        )
        mean = totals * scale[g][:, 0:1]
        base = 0
        for c, (rows, _) in enumerate(CHUNKS):
            n = 4 * rows
            lo, hi = mean[base : base + n], mean[base + n : base + 2 * n]
            packed = jnp.concatenate(
                [lo[:, :MAIN], hi[:, :MAIN], lo[:, MAIN:], hi[:, MAIN:]], axis=1
            )
            pooled[c][pl.ds(n * g, n), :] = packed.astype(BF)
            base += 2 * n

    def choose(c):
        rows = CHUNKS[c][0]
        chosen = jnp.dot(pick[c][...], pooled[c][...], preferred_element_type=F32)
        snd[c][...] = chosen.reshape(GROUPS, rows, 2 * FH).astype(BF)
        arr[c][pl.ds(me, 1)] = snd[c][pl.ds(me, 1)]

    def send_all(src, dst, send_sem, recv_sem):
        for to in targets:
            pltpu.make_async_remote_copy(
                src_ref=src.at[pl.ds(to, 1)],
                dst_ref=dst.at[pl.ds(me, 1)],
                send_sem=send_sem,
                recv_sem=recv_sem,
                device_id=(to, core),
                device_id_type=MESH,
            ).start()

    choose(0)
    pl.semaphore_wait(barrier, GROUPS)
    send_all(meta_out, meta_in, meta_s, meta_r)
    send_all(snd[0], arr[0], a_s.at[0], a_r.at[0])
    for c in range(1, EARLY):
        choose(c)
        send_all(snd[c], arr[c], a_s.at[c], a_r.at[c])

    def whole(src, dst, send_sem, recv_sem):
        return pltpu.make_async_remote_copy(
            src_ref=src.at[pl.ds(0, GROUPS - 1)],
            dst_ref=dst.at[pl.ds(0, GROUPS - 1)],
            send_sem=send_sem,
            recv_sem=recv_sem,
            device_id=(me, other),
            device_id_type=MESH,
        )

    def to_partner(src, dst, send_sem, recv_sem):
        return pltpu.make_async_remote_copy(
            src_ref=src,
            dst_ref=dst,
            send_sem=send_sem,
            recv_sem=recv_sem,
            device_id=(me, other),
            device_id_type=MESH,
        )

    whole(meta_out, meta_in, meta_s, meta_r).wait_recv()

    for c, (rows, _) in enumerate(CHUNKS):
        lanes = GROUPS * rows
        wins = 2 * rows
        spread = jnp.where(
            div(iota((GROUPS, lanes), 1), rows) == iota((GROUPS, lanes), 0), 1.0, 0.0
        )
        slots = lax.dot_general(
            meta_in[...].reshape(GROUPS, 128).astype(F32).astype(BF),
            spread.astype(BF),
            (((0,), (0,)), ((), ())),
            preferred_element_type=F32,
        )
        shape = (SAMP * wins, lanes)
        mine = slots[0:1] == (div(iota(shape, 0), wins) + 1).astype(F32)
        win = mod(iota(shape, 0), wins)
        lane_r = mod(iota(shape, 1), rows)
        for h in range(2):
            mask = jnp.where(mine & (win == h * rows + lane_r), 1.0, 0.0)
            place[c][:, pl.ds(h * lanes, lanes)] = mask.astype(BF)

    def gather(c):
        rows = CHUNKS[c][0]
        lanes = GROUPS * rows
        whole(snd[c], arr[c], a_s.at[c], a_r.at[c]).wait_recv()
        block = arr[c][...].reshape(lanes, 2 * FH)
        tails = block[:, 2 * MAIN :].astype(F32)
        low = iota((lanes, 128), 1) < FH - MAIN
        zero = jnp.zeros_like(tails)
        halves = [
            jnp.concatenate(
                [block[:, h * MAIN : (h + 1) * MAIN], jnp.where(low, *pair).astype(BF)], axis=1
            )
            for h, pair in enumerate(((tails, zero), (zero, tails)))
        ]
        placed = jnp.dot(
            place[c][...], jnp.concatenate(halves, axis=0), preferred_element_type=F32
        )
        xf[c][:, pl.ds(0, PAD)] = placed.astype(BF)
        swap = to_partner(
            xf[c].at[:, pl.ds(0, PAD)], xf[c].at[:, pl.ds(PAD, PAD)], x_s.at[c], x_r.at[c]
        )
        swap.start()
        return swap

    def layer1(c):
        total = SAMP * 2 * CHUNKS[c][0]
        for n in range(HID // 256):
            cols = pl.ds(n * 256, 256)
            pre = jnp.dot(xf[c][...], w1[:, cols], preferred_element_type=F32)
            pre = pre + b_first[cols].reshape(1, 256)
            hid[pl.ds(0, total), cols] = gelu(pre).astype(BF)

    def layer2(c, tiles):
        total = SAMP * 2 * CHUNKS[c][0]
        for n in tiles:
            cols = pl.ds(n * 256, 256)
            value = jnp.dot(hid[pl.ds(0, total), :], w2[:, cols], preferred_element_type=F32)
            value = value.astype(BF)
            if n < 4:
                ps[c][:, cols] = value
            elif n == 4:
                ps[c][:, pl.ds(1024, 128)] = value[:, :128]
                po[c][:, pl.ds(0, 128)] = value[:, 128:]
            else:
                po[c][:, pl.ds(n * 256 - OUT, 256)] = value

    def finish(c):
        rows, first = CHUNKS[c]
        for n in range(3):
            cols = pl.ds(n * 384, 384)
            summed = po[c][:, cols].astype(F32) + pr[c][:, cols].astype(F32)
            value = (summed + b_second[cols].reshape(1, 384)).reshape(SAMP, 2 * rows, 384)
            out[:, pl.ds(first, 2 * rows), cols] = value.astype(BF)

    swap = gather(0)
    for c in range(EARLY, len(CHUNKS)):
        choose(c)
        send_all(snd[c], arr[c], a_s.at[c], a_r.at[c])
    for copy in w_copies:
        copy.wait()
    pending = None
    for c in range(len(CHUNKS)):
        last = c == len(CHUNKS) - 1
        swap.wait()
        layer1(c)
        if not last:
            swap = gather(c + 1)
        if pending is not None:
            pending.wait()
        give = to_partner(ps[c], pr[c], p_s.at[c], p_r.at[c])
        layer2(c, range(5))
        if last:
            give.start()
        if pending is not None:
            finish(c - 1)
        layer2(c, range(5, 9))
        if not last:
            give.start()
        pending = give
    pending.wait()
    finish(len(CHUNKS) - 1)

    whole(meta_out, meta_in, meta_s, meta_r).wait_send()
    for c in range(len(CHUNKS)):
        whole(snd[c], arr[c], a_s.at[c], a_r.at[c]).wait_send()


def shards(encoded, counts, win_ids, dest_seq, dest_slot, w_first, b_first, w_second, b_second):
    vmem = pl.BlockSpec(memory_space=pltpu.VMEM)
    hbm = pl.BlockSpec(memory_space=pltpu.HBM)
    n = len(CHUNKS)
    sizes = [rows for rows, _ in CHUNKS]
    scratch = [pltpu.SMEM((SAMP,), I32)] * 3
    scratch += [
        pltpu.VMEM((SAMP, CAP), I32),
        pltpu.VMEM((HID,), F32),
        pltpu.VMEM((OUT,), F32),
        pltpu.VMEM((FH, SAMP * CAP), BF),
        pltpu.VMEM((2 * PAD, HID), BF),
        pltpu.VMEM((HID, 2 * OUT), BF),
    ]
    scratch += [pltpu.VMEM((GROUPS, 1, 128), I32)] * 2
    scratch += [pltpu.VMEM((SAMP * 2 * max(sizes), HID), BF)]
    scratch += [pltpu.VMEM((SAMP // 4, 128, 256), BF), pltpu.VMEM((SAMP // 4, 128, 128), F32)]
    scratch += [pltpu.VMEM((SAMP * r, 2 * FH), BF) for r in sizes]
    scratch += [pltpu.VMEM((GROUPS, r, 2 * FH), BF) for r in sizes] * 2
    scratch += [pltpu.VMEM((SAMP * 2 * r, 2 * PAD), BF) for r in sizes]
    scratch += [pltpu.VMEM((SAMP * 2 * r, OUT), BF) for r in sizes] * 3
    scratch += [pltpu.VMEM((SAMP * 2 * r, 2 * GROUPS * r), BF) for r in sizes]
    scratch += [pltpu.VMEM((GROUPS * r, SAMP * r), BF) for r in sizes]
    dma = pltpu.SemaphoreType.DMA
    scratch += [dma((6,)), dma, dma((8,)), dma, dma, dma((n,)), dma((n,)), dma((n,)), dma((n,)), dma((n,)), dma((n,))]
    result = pl.pallas_call(
        kernel,
        name="pool_place_project",
        out_shape=pltpu.VMEM((SAMP, BLOCK, OUT), BF),
        in_specs=[hbm] * 9,
        out_specs=vmem,
        scratch_shapes=scratch,
        compiler_params=pltpu.CompilerParams(
            collective_id=0, has_side_effects=True, vmem_limit_bytes=52 << 20
        ),
    )(
        counts, dest_seq, dest_slot, win_ids, b_first, b_second,
        encoded.T, w_first, w_second,
    )
    return result.reshape(SAMP * BLOCK, OUT)


def solution(mesh):
    placed = (
        P("dp", "tensor"),
        P("dp"),
        P("dp", None),
        P("dp"),
        P("dp"),
        P(None, "tensor"),
        P("tensor"),
        P("tensor", None),
        P("tensor"),
    )
    return jax.shard_map(
        shards, mesh=mesh, in_specs=placed, out_specs=P("dp", "tensor"), check_vma=False
    )
```

```python
import functools

import jax
import jax.numpy as jnp
from jax import lax
from jax.experimental import pallas as pl
from jax.experimental.pallas import tpu as pltpu
from jax.sharding import PartitionSpec as P

MESH = pl.DeviceIdType.MESH
BF = jnp.bfloat16
F32 = jnp.float32
I32 = jnp.int32

GROUPS = 64
SAMP = 32
CAP = 64
BLOCK = 32
FH = 576
MAIN = 512
OUT = 1152
HID = 2304
CHUNKS = tuple((2, 4 * c) for c in range(8))
LAG = 2
PAD = 640


def iota(shape, dim):
    return lax.broadcasted_iota(I32, shape, dim)


def div(x, n):
    return lax.shift_right_logical(x, jnp.int32(n.bit_length() - 1))


def mod(x, n):
    return lax.bitwise_and(x, jnp.int32(n - 1))


def hops(off):
    return sum(min(d, 4 - d) for d in off)


def peers(me):
    places = []
    for scale in (16, 4, 1):
        here = lax.rem(me // scale, 4)
        places.append([lax.rem(here + d, 4) * scale for d in range(4)])
    offsets = [(i // 16, i // 4 % 4, i % 4) for i in range(1, GROUPS)]
    done = []
    for off in sorted(offsets, key=lambda o: -hops(o)):
        for one in (off, tuple((4 - d) % 4 for d in off)):
            if one not in done:
                done.append(one)
    return [sum(places[i][d] for i, d in enumerate(off)) for off in done]


def gelu(x):
    half = 0.5 * x
    return half + half * jnp.tanh(x * (0.7978845608028654 + 0.035677408136300125 * (x * x)))


def kernel(*refs):
    n = len(CHUNKS)
    counts_in, seq_in, slot_in, win_in, b_first_in, b_second_in, enc, w_first, w_second, out = refs[:10]
    counts, dest_seq, dest_slot, win_ids, b_first, b_second, tok, w1, w2 = refs[10:19]
    meta_out, meta_in, hid, hot, scale = refs[19:24]
    pooled, snd, arr, xf, ps, pr, po, place, pick = (
        refs[24 + i * n : 24 + (i + 1) * n] for i in range(9)
    )
    in_sem, enc_sem, w_sem, meta_s, meta_r, a_s, a_r, x_s, x_r, p_s, p_r = refs[24 + 9 * n :]
    me = lax.axis_index("dp")
    core = lax.axis_index("tensor")
    other = 1 - core

    barrier = pltpu.get_barrier_semaphore()

    targets = peers(me)
    for to in targets:
        pl.semaphore_signal(barrier, inc=1, device_id=(to, core), device_id_type=MESH)
    pl.semaphore_signal(barrier, inc=1, device_id=(me, other), device_id_type=MESH)

    small = [
        pltpu.make_async_copy(src, dst, in_sem.at[i])
        for i, (src, dst) in enumerate(
            (
                (counts_in, counts),
                (seq_in, dest_seq),
                (slot_in, dest_slot),
                (win_in, win_ids),
                (b_first_in, b_first),
                (b_second_in, b_second),
            )
        )
    ]
    for copy in small:
        copy.start()
    enc_copy = pltpu.make_async_copy(enc, tok, enc_sem)
    enc_copy.start()

    w_copies = []
    for side, base in ((0, core * FH), (1, other * FH)):
        at = side * PAD
        w_copies += [(w_first.at[pl.ds(pl.multiple_of(base, 64), MAIN)], w1.at[pl.ds(at, MAIN)])]
        for twice in range(2):
            w_copies += [
                (
                    w_first.at[pl.ds(pl.multiple_of(base + MAIN, 64), 64)],
                    w1.at[pl.ds(at + MAIN + 64 * twice, 64)],
                )
            ]
    for at, base in ((0, other * OUT), (OUT, core * OUT)):
        for half in range(2):
            rows = pl.ds(half * (HID // 2), HID // 2)
            columns = pl.ds(pl.multiple_of(base, 128), OUT)
            w_copies.append((w_second.at[rows, columns], w2.at[rows, pl.ds(at, OUT)]))
    w_copies = [
        pltpu.make_async_copy(src, dst, w_sem.at[i]) for i, (src, dst) in enumerate(w_copies)
    ]

    for copy in small:
        copy.wait()
    row = iota((GROUPS, 128), 0)
    meta = jnp.zeros((GROUPS, 128), I32)
    for s in range(SAMP):
        meta = jnp.where(row == dest_seq[s], dest_slot[s] + 1, meta)
    meta_out[...] = meta.reshape(GROUPS, 1, 128)
    meta_in[pl.ds(me, 1)] = meta_out[pl.ds(me, 1)]

    ids = iota((SAMP, CAP), 1)
    srow = iota((SAMP, CAP), 0)
    limit = jnp.zeros((SAMP, CAP), I32)
    for s in range(SAMP):
        limit = jnp.where(srow == s, counts[s], limit)
    live = jnp.where(ids < limit, win_ids[...], -1)

    rho = iota((128, 256), 0)
    wmap = jnp.zeros((128, 256), I32)
    smap = jnp.zeros((128, 256), I32)
    base = 0
    for rows, first in CHUNKS:
        q = rho - base
        inside = (q >= 0) & (q < 8 * rows)
        h = div(q, 4 * rows)
        wmap = jnp.where(inside, first + h * rows + mod(q, rows), wmap)
        smap = jnp.where(inside, mod(div(q, rows), 4), smap)
        base += 8 * rows
    same = smap == div(iota((128, 256), 1), CAP)

    for g in range(SAMP // 4):
        line = jnp.concatenate([live[4 * g + i : 4 * g + i + 1, :] for i in range(4)], axis=1)
        onehot = jnp.where((wmap == line) & same, 1.0, 0.0).astype(F32)
        number = jnp.sum(onehot, axis=1, keepdims=True)
        hot[g] = onehot.astype(BF)
        scale[g] = jnp.broadcast_to(1.0 / jnp.maximum(number, 1.0), (128, 128))
    for c, (rows, _) in enumerate(CHUNKS):
        lanes = SAMP * rows
        where = jnp.zeros((8, lanes), I32)
        lane_s = div(iota((8, lanes), 1), rows)
        for s in range(SAMP):
            where = jnp.where(lane_s == s, dest_seq[s], where)
        shape = (GROUPS * rows, lanes)
        chosen = (div(iota(shape, 0), rows) == where[0:1]) & (
            mod(iota(shape, 0), rows) == mod(iota(shape, 1), rows)
        )
        pick[c][...] = jnp.where(chosen, 1.0, 0.0).astype(BF)

    enc_copy.wait()

    for g in range(SAMP // 4):
        totals = lax.dot_general(
            hot[g],
            tok[:, pl.ds(256 * g, 256)],
            (((1,), (1,)), ((), ())),
            preferred_element_type=F32,
        )
        mean = totals * scale[g][:, 0:1]
        base = 0
        for c, (rows, _) in enumerate(CHUNKS):
            n = 4 * rows
            lo, hi = mean[base : base + n], mean[base + n : base + 2 * n]
            packed = jnp.concatenate(
                [lo[:, :MAIN], hi[:, :MAIN], lo[:, MAIN:], hi[:, MAIN:]], axis=1
            )
            pooled[c][pl.ds(n * g, n), :] = packed.astype(BF)
            base += 2 * n

    def choose(c):
        rows = CHUNKS[c][0]
        chosen = jnp.dot(pick[c][...], pooled[c][...], preferred_element_type=F32)
        snd[c][...] = chosen.reshape(GROUPS, rows, 2 * FH).astype(BF)
        arr[c][pl.ds(me, 1)] = snd[c][pl.ds(me, 1)]

    def send_all(src, dst, send_sem, recv_sem):
        for to in targets:
            pltpu.make_async_remote_copy(
                src_ref=src.at[pl.ds(to, 1)],
                dst_ref=dst.at[pl.ds(me, 1)],
                send_sem=send_sem,
                recv_sem=recv_sem,
                device_id=(to, core),
                device_id_type=MESH,
            ).start()

    choose(0)
    pl.semaphore_wait(barrier, GROUPS)
    send_all(meta_out, meta_in, meta_s, meta_r)
    send_all(snd[0], arr[0], a_s.at[0], a_r.at[0])
    parts = [w_copies[0:3], w_copies[3:6]] + [w_copies[i : i + 1] for i in range(6, 10)]
    for c in range(1, len(CHUNKS) + LAG):
        if c < len(CHUNKS):
            choose(c)
        if c > LAG:
            send_all(snd[c - LAG], arr[c - LAG], a_s.at[c - LAG], a_r.at[c - LAG])
        if 0 <= c - 2 < len(parts):
            for copy in parts[c - 2]:
                copy.start()

    def whole(src, dst, send_sem, recv_sem):
        return pltpu.make_async_remote_copy(
            src_ref=src.at[pl.ds(0, GROUPS - 1)],
            dst_ref=dst.at[pl.ds(0, GROUPS - 1)],
            send_sem=send_sem,
            recv_sem=recv_sem,
            device_id=(me, other),
            device_id_type=MESH,
        )

    def to_partner(src, dst, send_sem, recv_sem):
        return pltpu.make_async_remote_copy(
            src_ref=src,
            dst_ref=dst,
            send_sem=send_sem,
            recv_sem=recv_sem,
            device_id=(me, other),
            device_id_type=MESH,
        )

    whole(meta_out, meta_in, meta_s, meta_r).wait_recv()

    for c, (rows, _) in enumerate(CHUNKS):
        lanes = GROUPS * rows
        wins = 2 * rows
        spread = jnp.where(
            div(iota((GROUPS, lanes), 1), rows) == iota((GROUPS, lanes), 0), 1.0, 0.0
        )
        slots = lax.dot_general(
            meta_in[...].reshape(GROUPS, 128).astype(F32).astype(BF),
            spread.astype(BF),
            (((0,), (0,)), ((), ())),
            preferred_element_type=F32,
        )
        shape = (SAMP * wins, lanes)
        mine = slots[0:1] == (div(iota(shape, 0), wins) + 1).astype(F32)
        win = mod(iota(shape, 0), wins)
        lane_r = mod(iota(shape, 1), rows)
        for h in range(2):
            mask = jnp.where(mine & (win == h * rows + lane_r), 1.0, 0.0)
            place[c][:, pl.ds(h * lanes, lanes)] = mask.astype(BF)

    def gather(c):
        rows = CHUNKS[c][0]
        lanes = GROUPS * rows
        whole(snd[c], arr[c], a_s.at[c], a_r.at[c]).wait_recv()
        block = arr[c][...].reshape(lanes, 2 * FH)
        tails = block[:, 2 * MAIN :].astype(F32)
        low = iota((lanes, 128), 1) < FH - MAIN
        zero = jnp.zeros_like(tails)
        halves = [
            jnp.concatenate(
                [block[:, h * MAIN : (h + 1) * MAIN], jnp.where(low, *pair).astype(BF)], axis=1
            )
            for h, pair in enumerate(((tails, zero), (zero, tails)))
        ]
        placed = jnp.dot(
            place[c][...], jnp.concatenate(halves, axis=0), preferred_element_type=F32
        )
        xf[c][:, pl.ds(0, PAD)] = placed.astype(BF)
        swap = to_partner(
            xf[c].at[:, pl.ds(0, PAD)], xf[c].at[:, pl.ds(PAD, PAD)], x_s.at[c], x_r.at[c]
        )
        swap.start()
        return swap

    def layer1(c):
        total = SAMP * 2 * CHUNKS[c][0]
        for n in range(HID // 256):
            cols = pl.ds(n * 256, 256)
            pre = jnp.dot(xf[c][...], w1[:, cols], preferred_element_type=F32)
            pre = pre + b_first[cols].reshape(1, 256)
            hid[pl.ds(0, total), cols] = gelu(pre).astype(BF)

    def layer2(c, tiles):
        total = SAMP * 2 * CHUNKS[c][0]
        for n in tiles:
            cols = pl.ds(n * 256, 256)
            value = jnp.dot(hid[pl.ds(0, total), :], w2[:, cols], preferred_element_type=F32)
            value = value.astype(BF)
            if n < 4:
                ps[c][:, cols] = value
            elif n == 4:
                ps[c][:, pl.ds(1024, 128)] = value[:, :128]
                po[c][:, pl.ds(0, 128)] = value[:, 128:]
            else:
                po[c][:, pl.ds(n * 256 - OUT, 256)] = value

    def finish(c):
        rows, first = CHUNKS[c]
        for n in range(3):
            cols = pl.ds(n * 384, 384)
            summed = po[c][:, cols].astype(F32) + pr[c][:, cols].astype(F32)
            value = (summed + b_second[cols].reshape(1, 384)).reshape(SAMP, 2 * rows, 384)
            out[:, pl.ds(first, 2 * rows), cols] = value.astype(BF)

    swap = gather(0)
    for copy in w_copies:
        copy.wait()
    pending = None
    for c in range(len(CHUNKS)):
        last = c == len(CHUNKS) - 1
        swap.wait()
        layer1(c)
        if not last:
            swap = gather(c + 1)
        if pending is not None:
            pending.wait()
        give = to_partner(ps[c], pr[c], p_s.at[c], p_r.at[c])
        layer2(c, range(5))
        if last:
            give.start()
        if pending is not None:
            finish(c - 1)
        layer2(c, range(5, 9))
        if not last:
            give.start()
        pending = give
    pending.wait()
    finish(len(CHUNKS) - 1)

    whole(meta_out, meta_in, meta_s, meta_r).wait_send()
    for c in range(len(CHUNKS)):
        whole(snd[c], arr[c], a_s.at[c], a_r.at[c]).wait_send()


def shards(encoded, counts, win_ids, dest_seq, dest_slot, w_first, b_first, w_second, b_second):
    vmem = pl.BlockSpec(memory_space=pltpu.VMEM)
    hbm = pl.BlockSpec(memory_space=pltpu.HBM)
    n = len(CHUNKS)
    sizes = [rows for rows, _ in CHUNKS]
    scratch = [pltpu.SMEM((SAMP,), I32)] * 3
    scratch += [
        pltpu.VMEM((SAMP, CAP), I32),
        pltpu.VMEM((HID,), F32),
        pltpu.VMEM((OUT,), F32),
        pltpu.VMEM((FH, SAMP * CAP), BF),
        pltpu.VMEM((2 * PAD, HID), BF),
        pltpu.VMEM((HID, 2 * OUT), BF),
    ]
    scratch += [pltpu.VMEM((GROUPS, 1, 128), I32)] * 2
    scratch += [pltpu.VMEM((SAMP * 2 * max(sizes), HID), BF)]
    scratch += [pltpu.VMEM((SAMP // 4, 128, 256), BF), pltpu.VMEM((SAMP // 4, 128, 128), F32)]
    scratch += [pltpu.VMEM((SAMP * r, 2 * FH), BF) for r in sizes]
    scratch += [pltpu.VMEM((GROUPS, r, 2 * FH), BF) for r in sizes] * 2
    scratch += [pltpu.VMEM((SAMP * 2 * r, 2 * PAD), BF) for r in sizes]
    scratch += [pltpu.VMEM((SAMP * 2 * r, OUT), BF) for r in sizes] * 3
    scratch += [pltpu.VMEM((SAMP * 2 * r, 2 * GROUPS * r), BF) for r in sizes]
    scratch += [pltpu.VMEM((GROUPS * r, SAMP * r), BF) for r in sizes]
    dma = pltpu.SemaphoreType.DMA
    scratch += [dma((6,)), dma, dma((10,)), dma, dma, dma((n,)), dma((n,)), dma((n,)), dma((n,)), dma((n,)), dma((n,))]
    result = pl.pallas_call(
        kernel,
        name="pool_place_project",
        out_shape=pltpu.VMEM((SAMP, BLOCK, OUT), BF),
        in_specs=[hbm] * 9,
        out_specs=vmem,
        scratch_shapes=scratch,
        compiler_params=pltpu.CompilerParams(
            collective_id=0, has_side_effects=True, vmem_limit_bytes=52 << 20
        ),
    )(
        counts, dest_seq, dest_slot, win_ids, b_first, b_second,
        encoded.T, w_first, w_second,
    )
    return result.reshape(SAMP * BLOCK, OUT)


def solution(mesh):
    placed = (
        P("dp", "tensor"),
        P("dp"),
        P("dp", None),
        P("dp"),
        P("dp"),
        P(None, "tensor"),
        P("tensor"),
        P("tensor", None),
        P("tensor"),
    )
    return jax.shard_map(
        shards, mesh=mesh, in_specs=placed, out_specs=P("dp", "tensor"), check_vma=False
    )
```
